32 devices in a mesh: rep: 4 (over x, y), dp: 8 (over z, core).
Axes of the slice: x: 2, y: 2, z: 4, core: 2. Of those that a mesh axis runs over, the one named last changes fastest.
Arguments:
- x: bfloat16 [32, 2048, 512], P(('rep', 'dp')), parts along dimension 0
- dy: bfloat16 [32, 2048, 512], P(('rep', 'dp')), parts along dimension 0
- wq: bfloat16 [2, 512, 512], P(None, 'dp')
- wk: bfloat16 [2, 512, 512], P(None, 'dp')
- wv: bfloat16 [2, 512, 512], P(None, 'dp')
- wo: bfloat16 [2, 512, 512], P(None, 'dp')
- w_gate: bfloat16 [2, 512, 2048], P(None, 'dp')
- w_up: bfloat16 [2, 512, 2048], P(None, 'dp')
- w_down: bfloat16 [2, 2048, 512], P(None, 'dp')
- m_wq: float32 [2, 512, 512], P(None, 'dp')
- m_wk: float32 [2, 512, 512], P(None, 'dp')
- m_wv: float32 [2, 512, 512], P(None, 'dp')
- m_wo: float32 [2, 512, 512], P(None, 'dp')
- m_w_gate: float32 [2, 512, 2048], P(None, 'dp')
- m_w_up: float32 [2, 512, 2048], P(None, 'dp')
- m_w_down: float32 [2, 2048, 512], P(None, 'dp')
- v_wq: float32 [2, 512, 512], P(None, 'dp')
- v_wk: float32 [2, 512, 512], P(None, 'dp')
- v_wv: float32 [2, 512, 512], P(None, 'dp')
- v_wo: float32 [2, 512, 512], P(None, 'dp')
- v_w_gate: float32 [2, 512, 2048], P(None, 'dp')
- v_w_up: float32 [2, 512, 2048], P(None, 'dp')
- v_w_down: float32 [2, 2048, 512], P(None, 'dp')
Outputs:
- output 1: bfloat16 [8, 512, 512], P('rep', 'dp'), parts along dimension 0
- output 2: bfloat16 [8, 512, 512], P('rep', 'dp'), parts along dimension 0
- output 3: bfloat16 [8, 512, 512], P('rep', 'dp'), parts along dimension 0
- output 4: bfloat16 [8, 512, 512], P('rep', 'dp'), parts along dimension 0
- output 5: bfloat16 [8, 512, 2048], P('rep', 'dp'), parts along dimension 0
- output 6: bfloat16 [8, 512, 2048], P('rep', 'dp'), parts along dimension 0
- output 7: bfloat16 [8, 2048, 512], P('rep', 'dp'), parts along dimension 0
- output 8: float32 [8, 512, 512], P('rep', 'dp'), parts along dimension 0
- output 9: float32 [8, 512, 512], P('rep', 'dp'), parts along dimension 0
- output 10: float32 [8, 512, 512], P('rep', 'dp'), parts along dimension 0
- output 11: float32 [8, 512, 512], P('rep', 'dp'), parts along dimension 0
- output 12: float32 [8, 512, 2048], P('rep', 'dp'), parts along dimension 0
- output 13: float32 [8, 512, 2048], P('rep', 'dp'), parts along dimension 0
- output 14: float32 [8, 2048, 512], P('rep', 'dp'), parts along dimension 0
- output 15: float32 [8, 512, 512], P('rep', 'dp'), parts along dimension 0
- output 16: float32 [8, 512, 512], P('rep', 'dp'), parts along dimension 0
- output 17: float32 [8, 512, 512], P('rep', 'dp'), parts along dimension 0
- output 18: float32 [8, 512, 512], P('rep', 'dp'), parts along dimension 0
- output 19: float32 [8, 512, 2048], P('rep', 'dp'), parts along dimension 0
- output 20: float32 [8, 512, 2048], P('rep', 'dp'), parts along dimension 0
- output 21: float32 [8, 2048, 512], P('rep', 'dp'), parts along dimension 0
There are 4 independent parts. The reference program is written for one: setup_inputs(seed, part) draws one part's arguments, and reference() takes and returns one part's arrays. A program takes and returns all parts, laid end to end along the dimension named above; an argument that names none is the same for every part.
All inputs are finite; a program needn't handle non-finite values.
Results may differ from the reference program's by a relative error of at most 0.029.
Values are sent between devices in bfloat16 or wider.
A program may use at most 2 GiB of HBM per device.

```python
import jax
import jax.numpy as jnp
from jax import lax

SEQUENCES = 8
TOKENS = 2048
D = 512
HEADS = 2
KV_HEADS = 2
HEAD = 256
FF = 2048
LAYERS = 2
THETA = 10000
NAMES = ("wq", "wk", "wv", "wo", "w_gate", "w_up", "w_down")
SHAPES = {
    "wq": (LAYERS, D, HEADS * HEAD),
    "wk": (LAYERS, D, KV_HEADS * HEAD),
    "wv": (LAYERS, D, KV_HEADS * HEAD),
    "wo": (LAYERS, HEADS * HEAD, D),
    "w_gate": (LAYERS, D, FF),
    "w_up": (LAYERS, D, FF),
    "w_down": (LAYERS, FF, D),
}


def bump(key, n, height):
    away = (jnp.arange(n, dtype=jnp.int32) - jax.random.randint(key, (), 0, n, jnp.int32)) % n
    return jnp.where(away < n // 8, height, 1.0)


def together(key, own, strength):
    shared = jax.random.normal(key, own.shape[1:], jnp.float32)
    return (own + strength * shared) * lax.rsqrt(1 + strength * strength)


def setup_inputs(seed: int = 0, part: int = 0) -> dict:
    kx, kdy, ka, kb, kz, kf, kh, kl, *keys = jax.random.split(jax.random.key(seed), 8 + 3 * len(NAMES))
    kx, kdy, ka, kb = (jax.random.fold_in(k, part) for k in (kx, kdy, ka, kb))
    kw, km, kv = (keys[i::3] for i in range(3))
    shape = (SEQUENCES, TOKENS, D)
    much_x, much_dy = jax.random.uniform(kz, (2,), jnp.float32, 0.0, 1.0)
    loud = 2.0 ** jax.random.uniform(jax.random.fold_in(kz, 1), (), jnp.float32, -1.0, 2.0)
    layers = 2.0 ** jax.random.uniform(kl, (LAYERS, 1, 1), jnp.float32, -1.0, 1.0)
    times = {"wq": 1.0, "wk": 1.0, "wv": 2.0, "wo": layers, "w_gate": 1.0, "w_up": bump(kh, FF, 4.0), "w_down": layers}
    x = together(ka, jax.random.normal(kx, shape, jnp.float32), much_x) * bump(kf, D, 4.0)
    dy = together(kb, jax.random.normal(kdy, shape, jnp.float32), much_dy)
    drawn = {"x": x.astype(jnp.bfloat16), "dy": (loud * dy * (SEQUENCES * TOKENS) ** -0.5).astype(jnp.bfloat16)}
    for key, name in zip(kw, NAMES, strict=True):
        drawn[name] = (jax.random.normal(key, SHAPES[name], jnp.float32) * SHAPES[name][1] ** -0.5 * times[name]).astype(jnp.bfloat16)
    for key, name in zip(km, NAMES, strict=True):
        drawn[f"m_{name}"] = 0.1 * jax.random.normal(key, SHAPES[name], jnp.float32)
    for key, name in zip(kv, NAMES, strict=True):
        drawn[f"v_{name}"] = loud * loud * jax.random.uniform(key, SHAPES[name], jnp.float32, 0.2, 0.6)
    return drawn


def matmul(a, w):
    return jnp.dot(a, w, preferred_element_type=jnp.float32).astype(jnp.bfloat16)


def normed(h):
    wide = h.astype(jnp.float32)
    scale = lax.rsqrt(jnp.mean(wide**2, -1, keepdims=True) + 1e-6)
    return (wide * scale).astype(jnp.bfloat16)


def turned(t, theta):
    half = t.shape[-1] // 2
    angle = jnp.arange(t.shape[0], dtype=jnp.float32)[:, None] * theta ** (-jnp.arange(half, dtype=jnp.float32) / half)
    cos, sin = jnp.cos(angle)[:, None], jnp.sin(angle)[:, None]
    a, b = t[..., :half].astype(jnp.float32), t[..., half:].astype(jnp.float32)
    return jnp.concatenate([a * cos - b * sin, b * cos + a * sin], -1).astype(jnp.bfloat16)


def seen_by(q, k, v):
    tokens, kv = q.shape[0], k.shape[1]
    q = q.reshape(tokens, kv, -1, q.shape[-1])
    scores = jnp.einsum("tgsd,ugd->gstu", q.astype(jnp.float32), k.astype(jnp.float32)) * q.shape[-1] ** -0.5
    place = jnp.arange(tokens)
    weights = jax.nn.softmax(jnp.where(place[:, None] >= place, scores, -jnp.inf), -1).astype(jnp.bfloat16)
    return jnp.einsum("gstu,ugd->tgsd", weights.astype(jnp.float32), v.astype(jnp.float32)).astype(jnp.bfloat16).reshape(tokens, -1)


def layer(h, w):
    a = normed(h)
    q, k = (turned(matmul(a, w[name]).reshape(h.shape[0], -1, HEAD), THETA) for name in ("wq", "wk"))
    h = h + matmul(seen_by(q, k, matmul(a, w["wv"]).reshape(h.shape[0], -1, HEAD)), w["wo"])
    b = normed(h)
    gate = jnp.dot(b, w["w_gate"], preferred_element_type=jnp.float32)
    up = jnp.dot(b, w["w_up"], preferred_element_type=jnp.float32)
    return h + matmul((jax.nn.silu(gate) * up).astype(jnp.bfloat16), w["w_down"])


def adamw(w, m, v, g):
    m = 0.9 * m + 0.1 * g
    v = 0.95 * v + 0.05 * g * g
    step = m * lax.rsqrt(v + 1e-8) + 0.1 * w
    return (w - 0.02 * step).astype(jnp.bfloat16), m, v


def stack(weights, h):
    return lax.scan(lambda h, w: (layer(h, w), None), h, weights)[0]


def reference(x, dy, wq, wk, wv, wo, w_gate, w_up, w_down, m_wq, m_wk, m_wv, m_wo, m_w_gate, m_w_up, m_w_down, v_wq, v_wk, v_wv, v_wo, v_w_gate, v_w_up, v_w_down):
    weights = dict(zip(NAMES, (wq, wk, wv, wo, w_gate, w_up, w_down), strict=True))

    def take(so_far, sequence):
        h, by_y = sequence
        _, back = jax.vjp(stack, weights, h)
        by_weights, by_h = back(by_y)
        return jax.tree.map(lambda total, term: total + term.astype(jnp.float32), so_far, by_weights), by_h

    none_yet = {name: jnp.zeros(w.shape, jnp.float32) for name, w in weights.items()}
    by_weights, by_x = lax.scan(take, none_yet, (x, dy))
    gradients = [by_weights[name].astype(jnp.bfloat16).astype(jnp.float32) for name in NAMES]
    first = (m_wq, m_wk, m_wv, m_wo, m_w_gate, m_w_up, m_w_down)
    second = (v_wq, v_wk, v_wv, v_wo, v_w_gate, v_w_up, v_w_down)
    new = [adamw(weights[name].astype(jnp.float32), m, v, g) for name, m, v, g in zip(NAMES, first, second, gradients, strict=True)]
    return tuple(one[which] for which in range(3) for one in new)
```

```python
import functools

import jax
import jax.numpy as jnp
from jax import lax
from jax.experimental import pallas as pl
from jax.experimental.pallas import tpu as pltpu
from jax.sharding import PartitionSpec as P


HEAD = 256
THETA = 10000
LOG2E = 1.4426950408889634
VMEM = 60 * 2**20
STRIP = 512
LOW, WIDE = jnp.bfloat16, jnp.float32


def _dot(a, b, ca, cb):
    return lax.dot_general(a, b, (((ca,), (cb,)), ((), ())), preferred_element_type=WIDE)


def _normed(h):
    wide = h.astype(WIDE)
    scale = lax.rsqrt(jnp.mean(wide * wide, -1, keepdims=True) + 1e-6)
    return wide, scale, (wide * scale).astype(LOW)


def _norm_back(wide, scale, by_out):
    along = jnp.mean(by_out * wide, -1, keepdims=True)
    return scale * by_out - wide * (scale * scale * scale * along)


def _attention(h_ref, w_ref, cos_ref, sin_ref, q_ref, k_ref, v_ref, o_ref, lse_ref, vt_s):
    tokens, d = h_ref.shape
    heads, half = d // HEAD, HEAD // 2
    e = HEAD**-0.5 * LOG2E
    for at in range(0, tokens, STRIP):
        rows = slice(at, at + STRIP)
        _, _, a = _normed(h_ref[rows, :])
        cos, sin = cos_ref[rows, :], sin_ref[rows, :]
        for part, ref in enumerate((q_ref, k_ref)):
            t = _dot(a, w_ref[:, part * d : (part + 1) * d], 1, 0).astype(LOW).astype(WIDE)
            for i in range(heads):
                x, y = t[:, i * HEAD : i * HEAD + half], t[:, i * HEAD + half : (i + 1) * HEAD]
                ref[rows, i * HEAD : i * HEAD + half] = (x * cos - y * sin).astype(LOW)
                ref[rows, i * HEAD + half : (i + 1) * HEAD] = (y * cos + x * sin).astype(LOW)
        v = _dot(a, w_ref[:, 2 * d : 3 * d], 1, 0).astype(LOW)
        v_ref[rows, :] = v
        vt_s[:, rows] = v.T
    seen = lax.broadcasted_iota(jnp.int32, (STRIP, STRIP), 0) <= lax.broadcasted_iota(jnp.int32, (STRIP, STRIP), 1)
    for at in range(0, tokens, STRIP):
        rows = slice(at, at + STRIP)
        for i in range(heads):
            mine = slice(i * HEAD, (i + 1) * HEAD)
            q = q_ref[rows, mine]
            keys = range(0, at + STRIP, STRIP)
            scores = [_dot(k_ref[j : j + STRIP, mine], q, 1, 1) for j in keys]
            scores[-1] = jnp.where(seen, scores[-1], -1e30)
            top = functools.reduce(jnp.maximum, [s.max(axis=0, keepdims=True) for s in scores])
            weights = [jnp.exp2((s - top) * e) for s in scores]
            total = sum(p.sum(axis=0, keepdims=True) for p in weights)
            out = sum(_dot(vt_s[mine, j : j + STRIP], p.astype(LOW), 1, 0) for j, p in zip(keys, weights))
            o_ref[rows, mine] = (out * (1 / total)).T.astype(LOW)
            lse_ref[i : i + 1, rows] = top * e + jnp.log(total) * LOG2E


def _attention_back(h_ref, by_ref, q_ref, k_ref, v_ref, o_ref, lse_ref, w_ref, cos_ref, sin_ref, out_ref, dw_ref,
                    do_s, kt_s, dk_s, dv_s, parts_s):
    tokens, d = h_ref.shape
    heads, half = d // HEAD, HEAD // 2
    scale = HEAD**-0.5
    e = scale * LOG2E
    strips = [slice(at, at + STRIP) for at in range(0, tokens, STRIP)]
    for rows in strips:
        do_s[rows, :] = _dot(by_ref[rows, :], w_ref[:, 3 * d : 4 * d], 1, 1).astype(LOW)
        kt_s[:, rows] = k_ref[rows, :].T
    dw_ref[:, 3 * d : 4 * d] = _dot(o_ref[...].T, by_ref[...], 1, 0).astype(LOW)
    seen = lax.broadcasted_iota(jnp.int32, (STRIP, STRIP), 0) <= lax.broadcasted_iota(jnp.int32, (STRIP, STRIP), 1)

    def turn_back(x, i, rows, part):
        x, y = x[:, :half].astype(LOW).astype(WIDE), x[:, half:].astype(LOW).astype(WIDE)
        cos, sin = cos_ref[rows, :], sin_ref[rows, :]
        at = part * d + i * HEAD
        parts_s[rows, at : at + half] = (x * cos + y * sin).astype(LOW)
        parts_s[rows, at + half : at + HEAD] = (y * cos - x * sin).astype(LOW)

    for n, rows in enumerate(strips):
        for i in range(heads):
            mine = slice(i * HEAD, (i + 1) * HEAD)
            q, do = q_ref[rows, mine], do_s[rows, mine]
            lse = lse_ref[i : i + 1, rows]
            delta = (do.astype(WIDE) * o_ref[rows, mine].astype(WIDE)).T.sum(axis=0, keepdims=True)
            dq = None
            for m, keys in enumerate(strips[: n + 1]):
                p = jnp.exp2(_dot(k_ref[keys, mine], q, 1, 1) * e - lse)
                if m == n:
                    p = jnp.where(seen, p, 0.0)
                dp = _dot(v_ref[keys, mine], do, 1, 1)
                ds = (p * (dp - delta)).astype(LOW)
                dv, dk = _dot(p.astype(LOW), do, 1, 0), _dot(ds, q, 1, 0)
                if m == n:
                    dv_s[keys, mine], dk_s[keys, mine] = dv, dk
                else:
                    dv_s[keys, mine] += dv
                    dk_s[keys, mine] += dk
                term = _dot(kt_s[mine, keys], ds, 1, 0)
                dq = term if dq is None else dq + term
            turn_back((dq * scale).T, i, rows, 0)
    for rows in strips:
        for i in range(heads):
            turn_back(dk_s[rows, i * HEAD : (i + 1) * HEAD] * scale, i, rows, 1)
        parts_s[rows, 2 * d : 3 * d] = dv_s[rows, :].astype(LOW)
        wide, r, a = _normed(h_ref[rows, :])
        do_s[rows, :] = a
        by_a = _dot(parts_s[rows, :], w_ref[:, : 3 * d], 1, 1).astype(LOW).astype(WIDE)
        back = _norm_back(wide, r, by_a).astype(LOW)
        out_ref[rows, :] = (by_ref[rows, :].astype(WIDE) + back.astype(WIDE)).astype(LOW)
    a_t = do_s[...].T
    for part in range(3):
        at = slice(part * d, (part + 1) * d)
        dw_ref[:, at] = _dot(a_t, parts_s[:, at], 1, 0).astype(LOW)


def _w_down(w_ref, wd_s, group):
    d, ff = w_ref.shape[0], wd_s.shape[0]
    own = d // group
    for dev in range(group):
        for j in range(ff // d):
            to = dev * (ff // group) + j * own
            wd_s[to : to + own, :] = w_ref[dev * own : (dev + 1) * own, 2 * ff + j * d : 2 * ff + (j + 1) * d]


def _mlp(h_ref, o_ref, wo_ref, w_ref, mid_ref, out_ref, wd_s, *, group):
    d, ff = w_ref.shape[0], wd_s.shape[0]

    @pl.when(pl.program_id(0) == 0)
    def _():
        _w_down(w_ref, wd_s, group)

    mid = (h_ref[...].astype(WIDE) + _dot(o_ref[...], wo_ref[...], 1, 0).astype(LOW).astype(WIDE)).astype(LOW)
    mid_ref[...] = mid
    _, _, b = _normed(mid)
    total = None
    for c in range(0, ff, d):
        gate = _dot(b, w_ref[:, c : c + d], 1, 0)
        up = _dot(b, w_ref[:, ff + c : ff + c + d], 1, 0)
        act = (gate * jax.nn.sigmoid(gate) * up).astype(LOW)
        term = _dot(act, wd_s[c : c + d, :], 1, 0)
        total = term if total is None else total + term
    out_ref[...] = (mid.astype(WIDE) + total.astype(LOW).astype(WIDE)).astype(LOW)


def _mlp_back(h_ref, by_ref, w_ref, out_ref, dw_ref, wd_s, dg_s, du_s, dd_s, *, group):
    d, ff = w_ref.shape[0], wd_s.shape[0]
    step = pl.program_id(0)

    @pl.when(step == 0)
    def _():
        _w_down(w_ref, wd_s, group)
        dg_s[...] = jnp.zeros_like(dg_s)
        du_s[...] = jnp.zeros_like(du_s)
        dd_s[...] = jnp.zeros_like(dd_s)

    by = by_ref[...]
    wide, r, b = _normed(h_ref[...])
    b_t, by_t = b.T, by.T
    by_b = None
    for c in range(0, ff, d):
        cols = slice(c, c + d)
        wg, wu = w_ref[:, c : c + d], w_ref[:, ff + c : ff + c + d]
        gate, up = _dot(b, wg, 1, 0), _dot(b, wu, 1, 0)
        by_act = _dot(by, wd_s[cols, :], 1, 1).astype(LOW).astype(WIDE)
        sig = jax.nn.sigmoid(gate)
        silu = gate * sig
        dd_s[:, cols] += _dot(by_t, (silu * up).astype(LOW), 1, 0)
        du = (by_act * silu).astype(LOW)
        dg = (by_act * up * (sig * (1.0 + gate * (1.0 - sig)))).astype(LOW)
        dg_s[:, cols] += _dot(b_t, dg, 1, 0)
        du_s[:, cols] += _dot(b_t, du, 1, 0)
        term = _dot(dg, wg, 1, 1) + _dot(du, wu, 1, 1)
        by_b = term if by_b is None else by_b + term
    back = _norm_back(wide, r, by_b.astype(LOW).astype(WIDE)).astype(LOW)
    out_ref[...] = (by.astype(WIDE) + back.astype(WIDE)).astype(LOW)

    @pl.when(step == pl.num_programs(0) - 1)
    def _():
        own, each = d // group, ff // group
        for c in range(0, ff, d):
            cols = slice(c, c + d)
            dw_ref[:, c : c + d] = dg_s[:, cols].astype(LOW)
            dw_ref[:, ff + c : ff + c + d] = du_s[:, cols].astype(LOW)
            down = dd_s[:, cols].T.astype(LOW)
            for at in range(0, d, own):
                dev, j = (c + at) // each, (c + at) % each // own
                dw_ref[dev * own : (dev + 1) * own, 2 * ff + j * d : 2 * ff + (j + 1) * d] = down[at : at + own, :]


def _like(shape, dtype=LOW):
    return jax.ShapeDtypeStruct(shape, dtype)


def _cost(flops, exps, *arrays):
    return pl.CostEstimate(flops=flops, transcendentals=exps, bytes_accessed=sum(a.size * a.dtype.itemsize for a in arrays))


def attention(h, w, cos, sin):
    t, d = h.shape
    outs = [_like((t, d))] * 4 + [_like((d // HEAD, t), WIDE)]
    pairs = t * (t + STRIP) // 2
    return pl.pallas_call(
        _attention, out_shape=outs, scratch_shapes=[pltpu.VMEM((d, t), LOW)],
        compiler_params=pltpu.CompilerParams(vmem_limit_bytes=VMEM),
        cost_estimate=_cost(2 * t * d * 3 * d + 4 * pairs * d, pairs * (d // HEAD), h, w, cos, sin, *outs),
    )(h, w, cos, sin)


def attention_back(h, by, q, k, v, o, lse, w, cos, sin):
    t, d = h.shape
    outs = [_like((t, d)), _like(w.shape)]
    pairs = t * (t + STRIP) // 2
    given = (h, by, q, k, v, o, lse, w, cos, sin)
    return pl.pallas_call(
        _attention_back, out_shape=outs,
        scratch_shapes=[pltpu.VMEM((t, d), LOW), pltpu.VMEM((d, t), LOW), pltpu.VMEM((t, d), WIDE), pltpu.VMEM((t, d), WIDE),
                        pltpu.VMEM((t, 3 * d), LOW)],
        compiler_params=pltpu.CompilerParams(vmem_limit_bytes=VMEM),
        cost_estimate=_cost(2 * t * d * 8 * d + 10 * pairs * d, pairs * (d // HEAD), *given, *outs),
    )(*given)


def mlp(h, o, wa, wm, group):
    t, d = h.shape
    ff = wm.shape[1] // 3
    rows = pl.BlockSpec((STRIP, d), lambda n: (n, 0))
    whole = pl.BlockSpec(wm.shape, lambda n: (0, 0))
    outs = [_like((t, d))] * 2
    return pl.pallas_call(
        functools.partial(_mlp, group=group), grid=(t // STRIP,), out_shape=outs,
        in_specs=[rows, rows, pl.BlockSpec((d, d), lambda n: (0, 3)), whole], out_specs=[rows, rows],
        scratch_shapes=[pltpu.VMEM((ff, d), LOW)],
        compiler_params=pltpu.CompilerParams(dimension_semantics=("arbitrary",), vmem_limit_bytes=VMEM),
        cost_estimate=_cost(2 * t * d * (d + 3 * ff), t * ff, h, o, wm, *outs),
    )(h, o, wa, wm)


def mlp_back(h, by, wm, group):
    t, d = h.shape
    ff = wm.shape[1] // 3
    rows = pl.BlockSpec((STRIP, d), lambda n: (n, 0))
    whole = pl.BlockSpec(wm.shape, lambda n: (0, 0))
    outs = [_like((t, d)), _like(wm.shape)]
    return pl.pallas_call(
        functools.partial(_mlp_back, group=group), grid=(t // STRIP,), out_shape=outs,
        in_specs=[rows, rows, whole], out_specs=[rows, whole],
        scratch_shapes=[pltpu.VMEM((ff, d), LOW)] + [pltpu.VMEM((d, ff), WIDE)] * 3,
        compiler_params=pltpu.CompilerParams(dimension_semantics=("arbitrary",), vmem_limit_bytes=VMEM),
        cost_estimate=_cost(2 * t * d * 8 * ff, t * ff, h, by, wm, *outs),
    )(h, by, wm)


def angles(tokens):
    half = HEAD // 2
    angle = jnp.arange(tokens, dtype=WIDE)[:, None] * THETA ** (-jnp.arange(half, dtype=WIDE) / half)
    return jnp.cos(angle), jnp.sin(angle)


def adamw(w, m, v, g):
    m = 0.9 * m + 0.1 * g
    v = 0.95 * v + 0.05 * g * g
    step = m * lax.rsqrt(v + 1e-8) + 0.1 * w
    return (w - 0.02 * step).astype(LOW), m, v


def solution(mesh):
    group = mesh.shape["dp"]

    def step(x, dy, *arrays):
        weights, m, v = (arrays[i : i + 7] for i in (0, 7, 14))
        wq, wk, wv, wo, w_gate, w_up, w_down = weights
        layers, own, d = wq.shape

        def side_by_side(w):
            return jnp.concatenate([w[at : at + own] for at in range(0, w.shape[0], own)], axis=1)

        held = []
        for n in range(layers):
            packs = (jnp.concatenate([w[n] for w in (wq, wk, wv, wo)], axis=1),
                     jnp.concatenate([w_gate[n], w_up[n], side_by_side(w_down[n])], axis=1))
            held.append([lax.all_gather(w, "dp", axis=0, tiled=True) for w in packs])
        cos, sin = angles(x.shape[1])
        h, kept = x[0], []
        for wa, wm in held:
            q, k, val, o, lse = attention(h, wa, cos, sin)
            mid, out = mlp(h, o, wa, wm, group)
            kept.append((h, q, k, val, o, lse, mid))
            h = out
        by, mine = dy[0], [None] * layers
        for n in reversed(range(layers)):
            wa, wm = held[n]
            h, q, k, val, o, lse, mid = kept[n]
            by, dwm = mlp_back(mid, by, wm, group)
            gm = lax.psum_scatter(dwm, "dp", scatter_dimension=0, tiled=True)
            by, dwa = attention_back(h, by, q, k, val, o, lse, wa, cos, sin)
            ga = lax.psum_scatter(dwa, "dp", scatter_dimension=0, tiled=True)
            ff = gm.shape[1] // 3
            down = jnp.concatenate([gm[:, at : at + d] for at in range(2 * ff, 3 * ff, d)], axis=0)
            mine[n] = [ga[:, i * d : (i + 1) * d] for i in range(4)] + [gm[:, :ff], gm[:, ff : 2 * ff], down]
        gradients = [jnp.stack([mine[n][i] for n in range(layers)]).astype(WIDE) for i in range(7)]
        new = [adamw(w.astype(WIDE), m, v, g) for w, m, v, g in zip(weights, m, v, gradients, strict=True)]
        return tuple(one[which] for which in range(3) for one in new)

    states, cut = P(("rep", "dp"), None, None), P(None, "dp", None)
    return jax.shard_map(
        step,
        mesh=mesh,
        in_specs=(states, states) + (cut,) * 21,
        out_specs=(P("rep", "dp", None),) * 21,
        check_vma=False,
    )
```
